32 devices in a mesh: subj: 8 (over z, core), var: 4 (over y, x).
Axes of the slice: x: 2, y: 2, z: 4, core: 2. Of those that a mesh axis runs over, the one named last changes fastest.
Arguments:
- traits: bfloat16 [16384, 256], P('subj', 'var'), may hold values from -6 to 6
- kin_tiles: bfloat16 [96, 256, 256], P('subj'), may hold values from -0.25 to 0.25
- kin_index: int32 [96, 2], P('subj'), may hold values from 0 to 63, as said below
- dosages: bfloat16 [16384, 3072], P('subj', 'var'), may hold values from 0 to 255, as said below
Outputs:
- scores: float32 [3072, 256], P(('var', 'subj'))
The draws below stay inside these ranges and needn't reach their ends.
Inputs may be any that keep to these rules, and one draw needn't show every extreme that they name: `kin_index`: rows t * 12 to (t + 1) * 12 - 1 hold tiles whose row block lies in t * 8 to (t + 1) * 8 - 1; every row block has its diagonal tile; counts per row block are uneven; a pair may repeat. `dosages`: whole numbers.
All inputs are finite; a program needn't handle non-finite values.
Results may differ from the reference program's by a relative error of at most 0.009.
Values may be sent and summed in bfloat16 or wider, within the bound.
A program may use at most 64 MiB of HBM per device.

```python
import jax
import jax.numpy as jnp
from jax import lax

K = 256
BLOCK = 256
SUBJ_DEV = 2048
VAR_DEV = 768
TILES_DEV = 12
NSUB = 16384
NVAR = 3072
NBLOCKS = 64
NTILES = 96
N_SUBJ = 8
N_VAR = 4


def draw_kin_index(key, part):
    per_dev = SUBJ_DEV // BLOCK
    extra = TILES_DEV - per_dev
    devices = jnp.arange(N_SUBJ, dtype=jnp.int32)
    diag = devices[:, None] * per_dev + jnp.arange(per_dev, dtype=jnp.int32)[None, :]
    key_rows, key_cols = jax.random.split(jax.random.fold_in(key, 11))
    extra_rows = devices[:, None] * per_dev + jax.random.randint(key_rows, (N_SUBJ, extra), 0, per_dev, dtype=jnp.int32)
    extra_cols = jax.random.randint(key_cols, (N_SUBJ, extra), 0, NBLOCKS, dtype=jnp.int32)
    rows_all = jnp.concatenate([diag, extra_rows], axis=1).reshape(-1)
    cols_all = jnp.concatenate([diag, extra_cols], axis=1).reshape(-1)
    return jnp.stack([rows_all, cols_all], axis=1).astype(jnp.int32)


def draw_dosages(key, part):
    codes = jax.random.randint(jax.random.fold_in(key, 23), (NSUB, NVAR), 0, 256, dtype=jnp.int32)
    return codes.astype(jnp.float32).astype(jnp.bfloat16)


def shard_levels(rng, shape, pieces, low, high):
    def one(dim, shards_of):
        heights = jax.random.uniform(jax.random.fold_in(jax.random.fold_in(rng, 6), dim), (shards_of,), jnp.float32, low / len(pieces), high / len(pieces))
        return jnp.repeat(jnp.exp(heights), shape[dim] // shards_of).reshape((-1,) + (1,) * (len(shape) - dim - 1))

    level = one(*pieces[0])
    for cut in pieces[1:]:
        level = level * one(*cut)
    return level


def gaussian(key, shape, spread, reach, pieces=(), kind=jnp.bfloat16):
    factor_of = shard_levels(key, shape, pieces, -0.22, 0.18) if pieces else 1.0
    drawn = jax.random.normal(key, shape, jnp.float32) * spread * factor_of
    return jnp.minimum(jnp.maximum(drawn, -reach), reach).astype(kind)


def setup_inputs(seed: int = 0) -> dict:
    splits = jax.random.split(jax.random.key(seed), 5)
    return {
        "traits": gaussian(splits[0], (NSUB, K), 1.0, 6.0, ((0, 8), (1, 4))),
        "kin_tiles": gaussian(splits[1], (NTILES, BLOCK, BLOCK), (2 * BLOCK) ** -0.5, 0.25, ((0, 8),)),
        "kin_index": draw_kin_index(jax.random.fold_in(splits[4], 71), 0),
        "dosages": draw_dosages(jax.random.fold_in(splits[4], 71), 0),
    }


def kinship_apply(field, kin_tiles, kin_index):
    width = field.shape[1]
    slabs = field.reshape(NBLOCKS, BLOCK, width)[kin_index[:, 1]].astype(jnp.float32)
    prods = jnp.einsum('tij,tjk->tik', kin_tiles.astype(jnp.float32), slabs)
    summed = jax.ops.segment_sum(prods, kin_index[:, 0], NBLOCKS)
    return summed.reshape(NSUB, width)

def reference(traits, kin_tiles, kin_index, dosages):
    first = kinship_apply(traits, kin_tiles, kin_index)
    first_sent = first.astype(jnp.bfloat16)
    second = kinship_apply(first_sent, kin_tiles, kin_index)
    base = traits.astype(jnp.float32)
    whitened = (0.6 * base + 0.5 * first + 0.3 * (2.0 * second - base)).astype(jnp.bfloat16)
    scale = 1.0 / (127.5 * jnp.sqrt(jnp.float32(NSUB)))
    blocks = dosages.reshape(NSUB, N_VAR, VAR_DEV).transpose(1, 0, 2)

    def score_block(block_dos):
        return lax.dot_general(block_dos, whitened, (((0,), (0,)), ((), ())), preferred_element_type=jnp.float32)
    scores = lax.map(score_block, blocks).reshape(NVAR, K)
    return scores * scale
```

```python
import functools
import math

import jax
import jax.numpy as jnp
from jax import lax
from jax.experimental import pallas as pl
from jax.experimental.pallas import tpu as pltpu
from jax.sharding import PartitionSpec as P

MESH = pl.DeviceIdType.MESH
CORES = 2


def plan_kernel(idx_ref, tab_ref, hot_ref):
    tiles = idx_ref.shape[1]
    blocks, others = hot_ref.shape
    row0 = lax.axis_index("subj") * blocks
    rows = [idx_ref[0, t] - row0 for t in range(tiles)]
    cols = [idx_ref[1, t] for t in range(tiles)]
    zero, one = jnp.int32(0), jnp.int32(1)
    first = []
    for t in range(tiles):
        flag = jnp.where(rows[t] + row0 == cols[t], one, zero)
        for u in range(t):
            flag = flag * jnp.where(rows[u] == rows[t], one - first[u], one)
        first.append(flag)
    for b in range(blocks):
        at = zero
        for t in range(tiles):
            at = at + jnp.where(rows[t] == b, first[t] * t, zero)
        tab_ref[0, b] = at
    ranks = []
    rank = zero
    for t in range(tiles):
        ranks.append(rank)
        rank = rank + (one - first[t])
    for e in range(others):
        tile, row, col = zero, zero, zero
        for t in range(tiles):
            hit = (one - first[t]) * jnp.where(ranks[t] == e, one, zero)
            tile = tile + hit * t
            row = row + hit * rows[t]
            col = col + hit * cols[t]
        tab_ref[1, e] = tile
        tab_ref[2, e] = col
        for b in range(blocks):
            hot_ref[b, e] = jnp.where(row == b, jnp.float32(1), jnp.float32(0))


def kernel(ns, nv, scale, tab_ref, hot_ref, t_ref, tiles_hbm, dos_hbm, o_ref,
           tiles, dos, gat1, gat2, prod, first, wide, part, pbuf, sbuf, rbuf,
           load_sem, zs, zr, ps, pr, ws, wr, qs, qr, rs, rr):
    s, v = lax.axis_index("subj"), lax.axis_index("var")
    nz = ns // CORES
    z, c = s // CORES, s % CORES
    partner = z * CORES + (1 - c)
    nt, blk = tiles.shape[0], tiles.shape[1]
    w, rows_here = t_ref.shape
    nb = rows_here // blk
    ne = nt - nb
    orows = o_ref.shape[0]

    load_t = pltpu.make_async_copy(tiles_hbm, tiles, load_sem.at[0])
    load_d = pltpu.make_async_copy(dos_hbm, dos, load_sem.at[1])
    load_t.start()
    load_d.start()

    barrier = pltpu.get_barrier_semaphore()
    for k in range(1, ns):
        pl.semaphore_signal(barrier, inc=1, device_id={"subj": lax.rem(s + k, ns)}, device_id_type=MESH)
    for k in range(1, nv):
        pl.semaphore_signal(barrier, inc=1, device_id={"var": lax.rem(v + k, nv)}, device_id_type=MESH)
    pl.semaphore_wait(barrier, ns - 1 + nv - 1)

    def gather(phase, gat, meanwhile):
        def blocks(dev):
            return gat.at[pl.ds(dev * nb, nb)]

        def up(k):
            return pltpu.make_async_remote_copy(
                src_ref=blocks(s - k * CORES), dst_ref=blocks(s - k * CORES),
                send_sem=zs.at[phase, 0, k], recv_sem=zr.at[phase, 0, k],
                device_id={"subj": s + CORES}, device_id_type=MESH)

        def down(k):
            return pltpu.make_async_remote_copy(
                src_ref=blocks(s + k * CORES), dst_ref=blocks(s + k * CORES),
                send_sem=zs.at[phase, 1, k], recv_sem=zr.at[phase, 1, k],
                device_id={"subj": s - CORES}, device_id_type=MESH)

        def across(k, sign):
            at = s + sign * k * CORES
            slot = k if sign > 0 else nz - 1 + k
            return pltpu.make_async_remote_copy(
                src_ref=blocks(at), dst_ref=blocks(at),
                send_sem=ps.at[phase, slot], recv_sem=pr.at[phase, slot],
                device_id={"subj": partner}, device_id_type=MESH)

        def landed(at, sem):
            pltpu.make_async_copy(blocks(at), blocks(at), sem).wait()

        @pl.when(z + 1 < nz)
        def _():
            up(0).start()

        @pl.when(z > 0)
        def _():
            down(0).start()

        across(0, 1).start()
        meanwhile()
        for k in range(nz - 1):
            @pl.when(z - 1 - k >= 0)
            def _():
                landed(s - (k + 1) * CORES, zr.at[phase, 0, k])
                if k + 1 < nz - 1:
                    @pl.when(z + 1 < nz)
                    def _():
                        up(k + 1).start()
                across(k + 1, -1).start()

            @pl.when(z + 1 + k < nz)
            def _():
                landed(s + (k + 1) * CORES, zr.at[phase, 1, k])
                if k + 1 < nz - 1:
                    @pl.when(z > 0)
                    def _():
                        down(k + 1).start()
                across(k + 1, 1).start()

        landed(partner, pr.at[phase, 0])
        for k in range(1, nz):
            @pl.when(z - k >= 0)
            def _():
                landed(partner - k * CORES, pr.at[phase, nz - 1 + k])

            @pl.when(z + k < nz)
            def _():
                landed(partner + k * CORES, pr.at[phase, k])

        def finish():
            across(0, 1).wait_send()
            for k in range(1, nz):
                @pl.when(z - k >= 0)
                def _():
                    across(k, -1).wait_send()

                @pl.when(z + k < nz)
                def _():
                    across(k, 1).wait_send()
            for k in range(nz - 1):
                @pl.when((z + 1 < nz) & (z - k >= 0))
                def _():
                    up(k).wait_send()

                @pl.when((z > 0) & (z + k < nz))
                def _():
                    down(k).wait_send()
        return finish

    nt_dims = (((1,), (1,)), ((), ()))

    def apply(field, tile):
        return lax.dot_general(field, tile, nt_dims, preferred_element_type=jnp.float32)

    def diagonals(gat, keep):
        for b in range(nb):
            keep[b] = apply(gat[s * nb + b], tiles[tab_ref[0, b]])

    def off_diagonals(gat):
        for e in range(ne):
            prod[e] = apply(gat[tab_ref[2, e]], tiles[tab_ref[1, e]])

    def total(keep, b):
        value = keep[b]
        for e in range(ne):
            value = value + hot_ref[b, e] * prod[e]
        return value

    for b in range(nb):
        gat1[s * nb + b] = t_ref[:, b * blk:(b + 1) * blk]

    def start1():
        load_t.wait()
        diagonals(gat1, first.at[0])

    finish1 = gather(0, gat1, start1)
    off_diagonals(gat1)
    for b in range(nb):
        value = total(first.at[0], b)
        first[0, b] = value
        gat2[s * nb + b] = value.astype(jnp.bfloat16)

    finish2 = gather(1, gat2, lambda: diagonals(gat2, first.at[1]))
    off_diagonals(gat2)
    mine = wide.at[pl.ds(pl.multiple_of(v * w, w), w)]
    for b in range(nb):
        at = slice(b * blk, (b + 1) * blk)
        base = t_ref[:, at].astype(jnp.float32)
        second = total(first.at[1], b)
        mine[:, at] = (
            0.6 * base + 0.5 * first[0, b] + 0.3 * (2.0 * second - base)
        ).astype(jnp.bfloat16)

    sends = []
    for k in range(1, nv):
        sends.append(pltpu.make_async_remote_copy(
            src_ref=mine, dst_ref=mine, send_sem=ws.at[k], recv_sem=wr.at[k],
            device_id={"var": lax.rem(v + k, nv)}, device_id_type=MESH))
        sends[-1].start()
    finish1()
    finish2()
    load_d.wait()
    for k in range(1, nv):
        sends[k - 1].wait()

    for lo in range(0, dos.shape[1], blk):
        got = jnp.dot(wide[...], dos[:, lo:lo + blk], preferred_element_type=jnp.float32)
        part[lo:lo + blk, :] = got.T

    pairs = []
    for q in range(nz):
        pairs.append(pltpu.make_async_remote_copy(
            src_ref=part.at[pl.ds((q * CORES + 1 - c) * orows, orows)], dst_ref=pbuf.at[q],
            send_sem=qs.at[q], recv_sem=qr.at[q],
            device_id={"subj": partner}, device_id_type=MESH))
        pairs[-1].start()
    for q in range(nz):
        pairs[q].wait()
    outs = []
    for k in range(1, nz):
        to = lax.rem(z + k, nz)
        sbuf[k] = (part[pl.ds((to * CORES + c) * orows, orows), :] + pbuf[to]).astype(jnp.bfloat16)
        outs.append(pltpu.make_async_remote_copy(
            src_ref=sbuf.at[k], dst_ref=rbuf.at[k], send_sem=rs.at[k], recv_sem=rr.at[k],
            device_id={"subj": to * CORES + c}, device_id_type=MESH))
        outs[-1].start()
    acc = part[pl.ds(s * orows, orows), :] + pbuf[z]
    for k in range(1, nz):
        outs[k - 1].wait()
        acc = acc + rbuf[k].astype(jnp.float32)
    o_ref[...] = acc * scale


def on_device(ns, nv, traits, kin_tiles, kin_index, dosages):
    rows_here, w = traits.shape
    nt, blk = kin_tiles.shape[:2]
    nb = rows_here // blk
    ne = nt - nb
    nz = ns // CORES
    var_dev = dosages.shape[1]
    orows = var_dev // ns
    k_all = w * nv
    bf16, f32 = jnp.bfloat16, jnp.float32
    dma = pltpu.SemaphoreType.DMA
    scale = 1.0 / (127.5 * math.sqrt(rows_here * ns))
    any_spec = pl.BlockSpec(memory_space=pl.ANY)
    vmem = pl.BlockSpec(memory_space=pltpu.VMEM)
    smem = pl.BlockSpec(memory_space=pltpu.SMEM)
    tab, hot = pl.pallas_call(
        plan_kernel,
        out_shape=(jax.ShapeDtypeStruct((3, max(nb, ne)), jnp.int32),
                   jax.ShapeDtypeStruct((nb, ne), f32)),
        in_specs=[smem],
        out_specs=(smem, smem),
    )(kin_index.T)
    return pl.pallas_call(
        functools.partial(kernel, ns, nv, scale),
        out_shape=jax.ShapeDtypeStruct((orows, k_all), f32),
        in_specs=[smem, smem, vmem, any_spec, any_spec],
        out_specs=vmem,
        scratch_shapes=[
            pltpu.VMEM((nt, blk, blk), bf16),
            pltpu.VMEM((rows_here, var_dev), bf16),
            pltpu.VMEM((ns * nb, w, blk), bf16),
            pltpu.VMEM((ns * nb, w, blk), bf16),
            pltpu.VMEM((ne, w, blk), f32),
            pltpu.VMEM((2, nb, w, blk), f32),
            pltpu.VMEM((k_all, rows_here), bf16),
            pltpu.VMEM((var_dev, k_all), f32),
            pltpu.VMEM((nz, orows, k_all), f32),
            pltpu.VMEM((nz, orows, k_all), bf16),
            pltpu.VMEM((nz, orows, k_all), bf16),
            dma((2,)),
            dma((2, 2, nz)), dma((2, 2, nz)),
            dma((2, 2 * nz)), dma((2, 2 * nz)),
            dma((nv,)), dma((nv,)),
            dma((nz,)), dma((nz,)),
            dma((nz,)), dma((nz,)),
        ],
        compiler_params=pltpu.CompilerParams(
            collective_id=0, has_side_effects=True, vmem_limit_bytes=60 * 1024 * 1024),
    )(tab, hot, traits.T, kin_tiles, dosages)


def solution(mesh):
    in_specs = (P("subj", "var"), P("subj", None, None), P("subj", None), P("subj", "var"))
    out_specs = P(("var", "subj"), None)
    body = functools.partial(on_device, mesh.shape["subj"], mesh.shape["var"])
    return jax.shard_map(
        body, mesh=mesh, in_specs=in_specs, out_specs=out_specs, check_vma=False
    )
```

```python
import functools
import math

import jax
import jax.numpy as jnp
from jax import lax
from jax.experimental import pallas as pl
from jax.experimental.pallas import tpu as pltpu
from jax.sharding import PartitionSpec as P

MESH = pl.DeviceIdType.MESH
CORES = 2


def plan_kernel(idx_ref, tab_ref, hot_ref):
    tiles = idx_ref.shape[1]
    blocks, others = hot_ref.shape
    row0 = lax.axis_index("subj") * blocks
    rows = [idx_ref[0, t] - row0 for t in range(tiles)]
    cols = [idx_ref[1, t] for t in range(tiles)]
    zero, one = jnp.int32(0), jnp.int32(1)
    first = []
    for t in range(tiles):
        flag = jnp.where(rows[t] + row0 == cols[t], one, zero)
        for u in range(t):
            flag = flag * jnp.where(rows[u] == rows[t], one - first[u], one)
        first.append(flag)
    for b in range(blocks):
        at = zero
        for t in range(tiles):
            at = at + jnp.where(rows[t] == b, first[t] * t, zero)
        tab_ref[0, b] = at
    ranks = []
    rank = zero
    for t in range(tiles):
        ranks.append(rank)
        rank = rank + (one - first[t])
    for e in range(others):
        tile, row, col = zero, zero, zero
        for t in range(tiles):
            hit = (one - first[t]) * jnp.where(ranks[t] == e, one, zero)
            tile = tile + hit * t
            row = row + hit * rows[t]
            col = col + hit * cols[t]
        tab_ref[1, e] = tile
        tab_ref[2, e] = col
        for b in range(blocks):
            hot_ref[b, e] = jnp.where(row == b, jnp.float32(1), jnp.float32(0))


def kernel(ns, nv, scale, tab_ref, hot_ref, t_ref, tiles_hbm, dos_hbm, o_ref,
           tiles, dos, turned, gat1, gat2, prod, first, wide, part, pbuf, sbuf, rbuf,
           load_sem, zs, zr, ps, pr, ws, wr, qs, qr, rs, rr):
    s, v = lax.axis_index("subj"), lax.axis_index("var")
    nz = ns // CORES
    z, c = s // CORES, s % CORES
    partner = z * CORES + (1 - c)
    nt, blk = tiles.shape[0], tiles.shape[1]
    w, rows_here = t_ref.shape
    nb = rows_here // blk
    ne = nt - nb
    orows = o_ref.shape[0]
    var_dev = dos.shape[1]

    load_t = pltpu.make_async_copy(tiles_hbm, tiles, load_sem.at[0])
    load_d = pltpu.make_async_copy(dos_hbm, dos, load_sem.at[1])
    load_t.start()
    load_d.start()

    barrier = pltpu.get_barrier_semaphore()
    pl.semaphore_signal(barrier, inc=1, device_id={"subj": partner}, device_id_type=MESH)
    for k in range(1, nz):
        pl.semaphore_signal(
            barrier, inc=1, device_id={"subj": lax.rem(z + k, nz) * CORES + c}, device_id_type=MESH)
    for k in range(1, nv):
        pl.semaphore_signal(barrier, inc=1, device_id={"var": lax.rem(v + k, nv)}, device_id_type=MESH)
    pl.semaphore_wait(barrier, 1 + nz - 1 + nv - 1)

    def turn(off):
        return lax.rem(z + off + nz, nz) * CORES

    def gather(phase, gat, meanwhile, later=lambda: None):
        parts = ((0, nb // 2), (nb // 2, nb - nb // 2))

        def piece(dev, half):
            return gat.at[pl.ds(dev * nb + parts[half][0], parts[half][1])]

        def hop(sign, dist, half):
            ref = piece(turn(-sign * (dist - 1)) + c, half)
            way = 0 if sign > 0 else 1
            return pltpu.make_async_remote_copy(
                src_ref=ref, dst_ref=ref,
                send_sem=zs.at[phase, way, dist, half], recv_sem=zr.at[phase, way, dist, half],
                device_id={"subj": turn(sign) + c}, device_id_type=MESH)

        def across(off, half):
            ref = piece(turn(off) + c, half)
            return pltpu.make_async_remote_copy(
                src_ref=ref, dst_ref=ref,
                send_sem=ps.at[phase, off % nz, half], recv_sem=pr.at[phase, off % nz, half],
                device_id={"subj": partner}, device_id_type=MESH)

        def landed(dev, half, sem):
            ref = piece(dev, half)
            pltpu.make_async_copy(ref, ref, sem).wait()

        steps = []
        for dist in range(1, nz // 2 + 1):
            if 2 * dist < nz:
                steps += [(1, dist, 0), (-1, dist, 1), (1, dist, 1), (-1, dist, 0)]
            else:
                steps += [(1, dist, 0), (-1, dist, 1)]
        for step in steps:
            if step[1] == 1:
                hop(*step).start()
        for half in range(2):
            across(0, half).start()
        meanwhile()
        for i, (sign, dist, half) in enumerate(steps):
            way = 0 if sign > 0 else 1
            landed(turn(-sign * dist) + c, half, zr.at[phase, way, dist, half])
            if (sign, dist + 1, half) in steps:
                hop(sign, dist + 1, half).start()
            across(-sign * dist, half).start()
            if i == 1:
                later()
        for off in range(nz):
            for half in range(2):
                landed(turn(off) + 1 - c, half, pr.at[phase, off, half])

        def finish():
            for off in range(nz):
                for half in range(2):
                    across(off, half).wait_send()
            for step in steps:
                hop(*step).wait_send()
        return finish

    nt_dims = (((1,), (1,)), ((), ()))

    def apply(field, tile):
        return lax.dot_general(field, tile, nt_dims, preferred_element_type=jnp.float32)

    def diagonals(gat, keep):
        for b in range(nb):
            keep[b] = apply(gat[s * nb + b], tiles[tab_ref[0, b]])

    def off_diagonals(gat):
        for e in range(ne):
            prod[e] = apply(gat[tab_ref[2, e]], tiles[tab_ref[1, e]])

    def total(keep, b):
        value = keep[b]
        for e in range(ne):
            value = value + hot_ref[b, e] * prod[e]
        return value

    for b in range(nb):
        gat1[s * nb + b] = t_ref[:, b * blk:(b + 1) * blk]

    def start1():
        load_t.wait()
        diagonals(gat1, first.at[0])

    finish1 = gather(0, gat1, start1)
    off_diagonals(gat1)
    for b in range(nb):
        value = total(first.at[0], b)
        first[0, b] = value
        gat2[s * nb + b] = value.astype(jnp.bfloat16)

    def turn_dosages():
        load_d.wait()
        for lo in range(0, var_dev, blk):
            for b in range(nb):
                turned[lo:lo + blk, b * blk:(b + 1) * blk] = dos[b * blk:(b + 1) * blk, lo:lo + blk].T

    finish2 = gather(1, gat2, lambda: diagonals(gat2, first.at[1]), turn_dosages)
    off_diagonals(gat2)
    spans = ((0, nb // 2), (nb // 2, nb))
    row_v = pl.ds(pl.multiple_of(v * w, w), w)
    sends = []
    for i, (b0, b1) in enumerate(spans):
        for b in range(b0, b1):
            at = slice(b * blk, (b + 1) * blk)
            base = t_ref[:, at].astype(jnp.float32)
            second = total(first.at[1], b)
            wide[row_v, at] = (
                0.6 * base + 0.5 * first[0, b] + 0.3 * (2.0 * second - base)
            ).astype(jnp.bfloat16)
        mine = wide.at[row_v, pl.ds(b0 * blk, (b1 - b0) * blk)]
        for k in range(1, nv):
            sends.append(pltpu.make_async_remote_copy(
                src_ref=mine, dst_ref=mine, send_sem=ws.at[i, k], recv_sem=wr.at[i, k],
                device_id={"var": lax.rem(v + k, nv)}, device_id_type=MESH))
            sends[-1].start()

    pairs = []
    for q in range(nz):
        pairs.append(pltpu.make_async_remote_copy(
            src_ref=part.at[pl.ds((q * CORES + 1 - c) * orows, orows)], dst_ref=pbuf.at[q],
            send_sem=qs.at[q], recv_sem=qr.at[q],
            device_id={"subj": partner}, device_id_type=MESH))
    sent = 0
    for i, (b0, b1) in enumerate(spans):
        for k in range(1, nv):
            sends[i * (nv - 1) + k - 1].wait_recv()
        for lo in range(0, var_dev, blk):
            got = apply(turned[lo:lo + blk, b0 * blk:b1 * blk], wide[:, b0 * blk:b1 * blk])
            if i == 0:
                part[lo:lo + blk, :] = got
                continue
            part[lo:lo + blk, :] += got
            while sent < nz and (sent + 1) * CORES * orows <= lo + blk:
                pairs[sent].start()
                sent += 1
    finish1()
    finish2()
    for copy in sends:
        copy.wait_send()
    for q in range(nz):
        pairs[q].wait()
    outs = []
    for k in range(1, nz):
        to = lax.rem(z + k, nz)
        sbuf[k] = (part[pl.ds((to * CORES + c) * orows, orows), :] + pbuf[to]).astype(jnp.bfloat16)
        outs.append(pltpu.make_async_remote_copy(
            src_ref=sbuf.at[k], dst_ref=rbuf.at[k], send_sem=rs.at[k], recv_sem=rr.at[k],
            device_id={"subj": to * CORES + c}, device_id_type=MESH))
        outs[-1].start()
    acc = part[pl.ds(s * orows, orows), :] + pbuf[z]
    for k in range(1, nz):
        outs[k - 1].wait()
        acc = acc + rbuf[k].astype(jnp.float32)
    o_ref[...] = acc * scale


def on_device(ns, nv, traits, kin_tiles, kin_index, dosages):
    rows_here, w = traits.shape
    nt, blk = kin_tiles.shape[:2]
    nb = rows_here // blk
    ne = nt - nb
    nz = ns // CORES
    var_dev = dosages.shape[1]
    orows = var_dev // ns
    k_all = w * nv
    bf16, f32 = jnp.bfloat16, jnp.float32
    dma = pltpu.SemaphoreType.DMA
    scale = 1.0 / (127.5 * math.sqrt(rows_here * ns))
    any_spec = pl.BlockSpec(memory_space=pl.ANY)
    vmem = pl.BlockSpec(memory_space=pltpu.VMEM)
    smem = pl.BlockSpec(memory_space=pltpu.SMEM)
    tab, hot = pl.pallas_call(
        plan_kernel,
        out_shape=(jax.ShapeDtypeStruct((3, max(nb, ne)), jnp.int32),
                   jax.ShapeDtypeStruct((nb, ne), f32)),
        in_specs=[smem],
        out_specs=(smem, smem),
    )(kin_index.T)
    return pl.pallas_call(
        functools.partial(kernel, ns, nv, scale),
        out_shape=jax.ShapeDtypeStruct((orows, k_all), f32),
        in_specs=[smem, smem, vmem, any_spec, any_spec],
        out_specs=vmem,
        scratch_shapes=[
            pltpu.VMEM((nt, blk, blk), bf16),
            pltpu.VMEM((rows_here, var_dev), bf16),
            pltpu.VMEM((var_dev, rows_here), bf16),
            pltpu.VMEM((ns * nb, w, blk), bf16),
            pltpu.VMEM((ns * nb, w, blk), bf16),
            pltpu.VMEM((ne, w, blk), f32),
            pltpu.VMEM((2, nb, w, blk), f32),
            pltpu.VMEM((k_all, rows_here), bf16),
            pltpu.VMEM((var_dev, k_all), f32),
            pltpu.VMEM((nz, orows, k_all), f32),
            pltpu.VMEM((nz, orows, k_all), bf16),
            pltpu.VMEM((nz, orows, k_all), bf16),
            dma((2,)),
            dma((2, 2, nz, 2)), dma((2, 2, nz, 2)),
            dma((2, nz, 2)), dma((2, nz, 2)),
            dma((2, nv)), dma((2, nv)),
            dma((nz,)), dma((nz,)),
            dma((nz,)), dma((nz,)),
        ],
        compiler_params=pltpu.CompilerParams(
            collective_id=0, has_side_effects=True, vmem_limit_bytes=60 * 1024 * 1024),
    )(tab, hot, traits.T, kin_tiles, dosages)


def solution(mesh):
    in_specs = (P("subj", "var"), P("subj", None, None), P("subj", None), P("subj", "var"))
    out_specs = P(("var", "subj"), None)
    body = functools.partial(on_device, mesh.shape["subj"], mesh.shape["var"])
    return jax.shard_map(
        body, mesh=mesh, in_specs=in_specs, out_specs=out_specs, check_vma=False
    )
```

```python
import functools
import math

import jax
import jax.numpy as jnp
from jax import lax
from jax.experimental import pallas as pl
from jax.experimental.pallas import tpu as pltpu
from jax.sharding import PartitionSpec as P

MESH = pl.DeviceIdType.MESH
CORES = 2


def plan_kernel(idx_ref, tab_ref, hot_ref):
    tiles = idx_ref.shape[1]
    blocks, others = hot_ref.shape
    row0 = lax.axis_index("subj") * blocks
    rows = [idx_ref[0, t] - row0 for t in range(tiles)]
    cols = [idx_ref[1, t] for t in range(tiles)]
    zero, one = jnp.int32(0), jnp.int32(1)
    first = []
    for t in range(tiles):
        flag = jnp.where(rows[t] + row0 == cols[t], one, zero)
        for u in range(t):
            flag = flag * jnp.where(rows[u] == rows[t], one - first[u], one)
        first.append(flag)
    for b in range(blocks):
        at = zero
        for t in range(tiles):
            at = at + jnp.where(rows[t] == b, first[t] * t, zero)
        tab_ref[0, b] = at
    ranks = []
    rank = zero
    for t in range(tiles):
        ranks.append(rank)
        rank = rank + (one - first[t])
    touched = [zero] * blocks
    for e in range(others):
        tile, row, col = zero, zero, zero
        for t in range(tiles):
            hit = (one - first[t]) * jnp.where(ranks[t] == e, one, zero)
            tile = tile + hit * t
            row = row + hit * rows[t]
            col = col + hit * cols[t]
        tab_ref[1, e] = tile
        tab_ref[2, e] = col
        for b in range(blocks):
            hot_ref[b, e] = jnp.where(row == b, jnp.float32(1), jnp.float32(0))
            touched[b] = jnp.where(row == b, one, touched[b])
    late = zero
    for b in range(blocks):
        late = late + touched[b]
    early_at, late_at = zero, blocks - late
    for b in range(blocks):
        slot = jnp.where(touched[b] == one, late_at, early_at)
        tab_ref[3, slot] = jnp.int32(b)
        late_at = late_at + touched[b]
        early_at = early_at + (one - touched[b])


def kernel(ns, nv, scale, tab_ref, hot_ref, t_ref, tiles_hbm, dos_hbm, o_ref,
           tiles, dos, turned, gat1, gat2, prod, first, wide, part, pbuf, sbuf, rbuf,
           load_sem, zs, zr, ps, pr, ws, wr, qs, qr, rs, rr):
    s, v = lax.axis_index("subj"), lax.axis_index("var")
    nz = ns // CORES
    z, c = s // CORES, s % CORES
    partner = z * CORES + (1 - c)
    nt, blk = tiles.shape[0], tiles.shape[1]
    w, rows_here = t_ref.shape
    nb = rows_here // blk
    ne = nt - nb
    orows = o_ref.shape[0]
    var_dev = dos.shape[2]

    load_t = pltpu.make_async_copy(tiles_hbm, tiles, load_sem.at[0])
    load_d = pltpu.make_async_copy(dos_hbm, dos, load_sem.at[1])
    load_t.start()
    load_d.start()

    barrier = pltpu.get_barrier_semaphore()
    pl.semaphore_signal(barrier, inc=1, device_id={"subj": partner}, device_id_type=MESH)
    for k in range(1, nz):
        pl.semaphore_signal(
            barrier, inc=1, device_id={"subj": lax.rem(z + k, nz) * CORES + c}, device_id_type=MESH)
    for k in range(1, nv):
        pl.semaphore_signal(barrier, inc=1, device_id={"var": lax.rem(v + k, nv)}, device_id_type=MESH)
    pl.semaphore_wait(barrier, 1 + nz - 1 + nv - 1)

    def turn(off):
        return lax.rem(z + off + nz, nz) * CORES

    def gather(phase, gat, meanwhile, later=lambda: None):
        parts = ((0, nb // 2), (nb // 2, nb - nb // 2))

        def piece(dev, half):
            return gat.at[pl.ds(dev * nb + parts[half][0], parts[half][1])]

        def hop(sign, dist, half):
            ref = piece(turn(-sign * (dist - 1)) + c, half)
            way = 0 if sign > 0 else 1
            return pltpu.make_async_remote_copy(
                src_ref=ref, dst_ref=ref,
                send_sem=zs.at[phase, way, dist, half], recv_sem=zr.at[phase, way, dist, half],
                device_id={"subj": turn(sign) + c}, device_id_type=MESH)

        def across(off, half):
            ref = piece(turn(off) + c, half)
            return pltpu.make_async_remote_copy(
                src_ref=ref, dst_ref=ref,
                send_sem=ps.at[phase, off % nz, half], recv_sem=pr.at[phase, off % nz, half],
                device_id={"subj": partner}, device_id_type=MESH)

        def landed(dev, half, sem):
            ref = piece(dev, half)
            pltpu.make_async_copy(ref, ref, sem).wait()

        steps = []
        for dist in range(1, nz // 2 + 1):
            if 2 * dist < nz:
                steps += [(1, dist, 0), (-1, dist, 1), (1, dist, 1), (-1, dist, 0)]
            else:
                steps += [(1, dist, 0), (-1, dist, 1)]
        for step in steps:
            if step[1] == 1:
                hop(*step).start()
        for half in range(2):
            across(0, half).start()
        meanwhile()
        for i, (sign, dist, half) in enumerate(steps):
            way = 0 if sign > 0 else 1
            landed(turn(-sign * dist) + c, half, zr.at[phase, way, dist, half])
            if (sign, dist + 1, half) in steps:
                hop(sign, dist + 1, half).start()
            across(-sign * dist, half).start()
            if i == 1:
                later()
        for off in range(nz):
            for half in range(2):
                landed(turn(off) + 1 - c, half, pr.at[phase, off, half])

        def finish():
            for off in range(nz):
                for half in range(2):
                    across(off, half).wait_send()
            for step in steps:
                hop(*step).wait_send()
        return finish

    nt_dims = (((1,), (1,)), ((), ()))

    def apply(field, tile):
        return lax.dot_general(field, tile, nt_dims, preferred_element_type=jnp.float32)

    def diagonals(gat, keep):
        for b in range(nb):
            keep[b] = apply(gat[s * nb + b], tiles[tab_ref[0, b]])

    def off_diagonals(gat):
        for e in range(ne):
            prod[e] = apply(gat[tab_ref[2, e]], tiles[tab_ref[1, e]])

    def total(keep, b):
        value = keep[b]
        for e in range(ne):
            value = value + hot_ref[b, e] * prod[e]
        return value

    for b in range(nb):
        gat1[s * nb + b] = t_ref[:, b * blk:(b + 1) * blk]

    def start1():
        load_t.wait()
        diagonals(gat1, first.at[0])

    finish1 = gather(0, gat1, start1)
    off_diagonals(gat1)
    for b in range(nb):
        value = total(first.at[0], b)
        first[0, b] = value
        gat2[s * nb + b] = value.astype(jnp.bfloat16)

    def turn_dosages():
        load_d.wait()
        for lo in range(0, var_dev, blk):
            for b in range(nb):
                turned[lo:lo + blk, b * blk:(b + 1) * blk] = dos[tab_ref[3, b], :, lo:lo + blk].T

    early = max(nb - ne, 0)
    spans = [span for span in ((0, early), (early, nb)) if span[0] < span[1]]
    row_v = pl.ds(pl.multiple_of(v * w, w), w)
    sends = []

    def whiten(b0, b1):
        for j in range(b0, b1):
            b = tab_ref[3, j]
            base = gat1[s * nb + b].astype(jnp.float32)
            second = first[1, b] if b1 <= early else total(first.at[1], b)
            wide[row_v, j * blk:(j + 1) * blk] = (
                0.6 * base + 0.5 * first[0, b] + 0.3 * (2.0 * second - base)
            ).astype(jnp.bfloat16)
        mine = wide.at[row_v, pl.ds(b0 * blk, (b1 - b0) * blk)]
        i = len(sends) // (nv - 1) if nv > 1 else 0
        for k in range(1, nv):
            sends.append(pltpu.make_async_remote_copy(
                src_ref=mine, dst_ref=mine, send_sem=ws.at[i, k], recv_sem=wr.at[i, k],
                device_id={"var": lax.rem(v + k, nv)}, device_id_type=MESH))
            sends[-1].start()

    def start2():
        diagonals(gat2, first.at[1])
        if early:
            whiten(0, early)

    finish2 = gather(1, gat2, start2, turn_dosages)
    off_diagonals(gat2)
    whiten(early, nb)

    pairs = []
    for q in range(nz):
        pairs.append(pltpu.make_async_remote_copy(
            src_ref=part.at[pl.ds((q * CORES + 1 - c) * orows, orows)], dst_ref=pbuf.at[q],
            send_sem=qs.at[q], recv_sem=qr.at[q],
            device_id={"subj": partner}, device_id_type=MESH))
    sent = 0
    for i, (b0, b1) in enumerate(spans):
        for k in range(1, nv):
            sends[i * (nv - 1) + k - 1].wait_recv()
        for lo in range(0, var_dev, blk):
            got = apply(turned[lo:lo + blk, b0 * blk:b1 * blk], wide[:, b0 * blk:b1 * blk])
            part[lo:lo + blk, :] = got if i == 0 else part[lo:lo + blk, :] + got
            if i + 1 < len(spans):
                continue
            while sent < nz and (sent + 1) * CORES * orows <= lo + blk:
                pairs[sent].start()
                sent += 1
    finish1()
    finish2()
    for copy in sends:
        copy.wait_send()
    for q in range(nz):
        pairs[q].wait()
    outs = []
    for k in range(1, nz):
        to = lax.rem(z + k, nz)
        sbuf[k] = (part[pl.ds((to * CORES + c) * orows, orows), :] + pbuf[to]).astype(jnp.bfloat16)
        outs.append(pltpu.make_async_remote_copy(
            src_ref=sbuf.at[k], dst_ref=rbuf.at[k], send_sem=rs.at[k], recv_sem=rr.at[k],
            device_id={"subj": to * CORES + c}, device_id_type=MESH))
        outs[-1].start()
    acc = part[pl.ds(s * orows, orows), :] + pbuf[z]
    for k in range(1, nz):
        outs[k - 1].wait()
        acc = acc + rbuf[k].astype(jnp.float32)
    o_ref[...] = acc * scale


def on_device(ns, nv, traits, kin_tiles, kin_index, dosages):
    rows_here, w = traits.shape
    nt, blk = kin_tiles.shape[:2]
    nb = rows_here // blk
    ne = nt - nb
    nz = ns // CORES
    var_dev = dosages.shape[1]
    orows = var_dev // ns
    k_all = w * nv
    bf16, f32 = jnp.bfloat16, jnp.float32
    dma = pltpu.SemaphoreType.DMA
    scale = 1.0 / (127.5 * math.sqrt(rows_here * ns))
    any_spec = pl.BlockSpec(memory_space=pl.ANY)
    vmem = pl.BlockSpec(memory_space=pltpu.VMEM)
    smem = pl.BlockSpec(memory_space=pltpu.SMEM)
    tab, hot = pl.pallas_call(
        plan_kernel,
        out_shape=(jax.ShapeDtypeStruct((4, max(nb, ne)), jnp.int32),
                   jax.ShapeDtypeStruct((nb, ne), f32)),
        in_specs=[smem],
        out_specs=(smem, smem),
    )(kin_index.T)
    return pl.pallas_call(
        functools.partial(kernel, ns, nv, scale),
        out_shape=jax.ShapeDtypeStruct((orows, k_all), f32),
        in_specs=[smem, smem, vmem, any_spec, any_spec],
        out_specs=vmem,
        scratch_shapes=[
            pltpu.VMEM((nt, blk, blk), bf16),
            pltpu.VMEM((nb, blk, var_dev), bf16),
            pltpu.VMEM((var_dev, rows_here), bf16),
            pltpu.VMEM((ns * nb, w, blk), bf16),
            pltpu.VMEM((ns * nb, w, blk), bf16),
            pltpu.VMEM((ne, w, blk), f32),
            pltpu.VMEM((2, nb, w, blk), f32),
            pltpu.VMEM((k_all, rows_here), bf16),
            pltpu.VMEM((var_dev, k_all), f32),
            pltpu.VMEM((nz, orows, k_all), f32),
            pltpu.VMEM((nz, orows, k_all), bf16),
            pltpu.VMEM((nz, orows, k_all), bf16),
            dma((2,)),
            dma((2, 2, nz, 2)), dma((2, 2, nz, 2)),
            dma((2, nz, 2)), dma((2, nz, 2)),
            dma((2, nv)), dma((2, nv)),
            dma((nz,)), dma((nz,)),
            dma((nz,)), dma((nz,)),
        ],
        compiler_params=pltpu.CompilerParams(
            collective_id=0, has_side_effects=True, vmem_limit_bytes=60 * 1024 * 1024),
    )(tab, hot, traits.T, kin_tiles, dosages.reshape(nb, blk, var_dev))


def solution(mesh):
    in_specs = (P("subj", "var"), P("subj", None, None), P("subj", None), P("subj", "var"))
    out_specs = P(("var", "subj"), None)
    body = functools.partial(on_device, mesh.shape["subj"], mesh.shape["var"])
    return jax.shard_map(
        body, mesh=mesh, in_specs=in_specs, out_specs=out_specs, check_vma=False
    )
```
